64 devices in a mesh: data: 4 (over x, y), dap: 16 (over z, core).
Axes of the slice: x: 2, y: 2, z: 8, core: 2. Of those that a mesh axis runs over, the one named last changes fastest.
The devices are a block of a 4x4x8 slice.
Arguments:
- z_one: bfloat16 [2048, 512, 128], P(('data', 'dap')), parts along dimension 0
- mask_one: int32 [2048, 512], P(('data', 'dap')), parts along dimension 0
- z_two: bfloat16 [2048, 512, 128], P(('data', 'dap')), parts along dimension 0
- mask_two: int32 [2048, 512], P(('data', 'dap')), parts along dimension 0
- norm_in: bfloat16 [2, 2, 128], replicated
- w_proj: bfloat16 [2, 128, 512], replicated
- w_gate: bfloat16 [2, 128, 128], replicated
- norm_mid: bfloat16 [2, 2, 128], replicated
- w_out: bfloat16 [2, 128, 128], replicated
Outputs:
- output 1: bfloat16 [2048, 512, 128], P(('data', 'dap')), parts along dimension 0
- output 2: bfloat16 [2048, 512, 128], P(('data', 'dap')), parts along dimension 0
There are 4 independent parts. The reference program is written for one: setup_inputs(seed, part) draws one part's arguments, and reference() takes and returns one part's arrays. A program takes and returns all parts, laid end to end along the dimension named above; an argument that names none is the same for every part.
All inputs are finite; a program needn't handle non-finite values.
Results may differ from the reference program's by a relative error of at most 0.00586416.
Values are sent between devices in bfloat16 or wider.
A program may use at most 768 MiB of HBM per device.

```python
import jax
import jax.numpy as jnp
from jax import lax

N = 512
CZ = 128
C = 128


def layer_norm(vals, ln_gain, ln_shift):
    vals = vals.astype(jnp.float32)
    row_mean = jnp.mean(vals, axis=-1, keepdims=True)
    centred = vals - row_mean
    row_var = jnp.mean(centred * centred, axis=-1, keepdims=True)
    return centred * lax.rsqrt(row_var + 1e-5) * ln_gain.astype(jnp.float32) + ln_shift.astype(jnp.float32)


def draw_mask(mask_key):
    residue_ok = (jax.random.randint(mask_key, (N,), 0, 20) != 0).astype(jnp.int32)
    return residue_ok[:, None] * residue_ok[None, :]


def setup_inputs(seed: int = 0, part: int = 0) -> dict:
    part_keys = jax.random.split(jax.random.fold_in(jax.random.key(seed), part), 4)
    shared_keys = jax.random.split(jax.random.key(seed + 1), 5)
    norm_base = jnp.array([1.0, 0.0], jnp.float32)[None, :, None]
    return {
        "z_one": jax.random.normal(part_keys[0], (N, N, CZ), jnp.float32).astype(jnp.bfloat16),
        "mask_one": draw_mask(part_keys[1]),
        "z_two": jax.random.normal(part_keys[2], (N, N, CZ), jnp.float32).astype(jnp.bfloat16),
        "mask_two": draw_mask(part_keys[3]),
        "norm_in": (0.3 * jax.random.normal(shared_keys[0], (2, 2, CZ), jnp.float32) + norm_base).astype(jnp.bfloat16),
        "w_proj": (jax.random.normal(shared_keys[1], (2, CZ, 4 * C), jnp.float32) * CZ ** -0.5).astype(jnp.bfloat16),
        "w_gate": (jax.random.normal(shared_keys[2], (2, CZ, CZ), jnp.float32) * CZ ** -0.5).astype(jnp.bfloat16),
        "norm_mid": (0.3 * jax.random.normal(shared_keys[3], (2, 2, C), jnp.float32) + norm_base).astype(jnp.bfloat16),
        "w_out": (jax.random.normal(shared_keys[4], (2, C, CZ), jnp.float32) * C ** -0.5).astype(jnp.bfloat16),
    }


def project_row(z_row, mask_row, norm_in, w_proj):
    x_row = layer_norm(z_row, norm_in[0], norm_in[1]).astype(jnp.bfloat16)
    projected = jnp.dot(x_row, w_proj, preferred_element_type=jnp.float32)
    keep_mask = mask_row.astype(jnp.float32)[:, None]
    a_row = keep_mask * jax.nn.sigmoid(projected[:, C:2 * C]) * projected[:, :C]
    b_row = keep_mask * jax.nn.sigmoid(projected[:, 3 * C:]) * projected[:, 2 * C:3 * C]
    return a_row.astype(jnp.bfloat16), b_row.astype(jnp.bfloat16)


def output_row(z_row, t_row, norm_in, w_gate, norm_mid, w_out):
    x_row = layer_norm(z_row, norm_in[0], norm_in[1]).astype(jnp.bfloat16)
    gate_val = jax.nn.sigmoid(jnp.dot(x_row, w_gate, preferred_element_type=jnp.float32))
    t_norm = layer_norm(t_row, norm_mid[0], norm_mid[1]).astype(jnp.bfloat16)
    update = jnp.dot(t_norm, w_out, preferred_element_type=jnp.float32)
    return (z_row.astype(jnp.float32) + gate_val * update).astype(jnp.bfloat16)


def tri_update(z_pair, pair_mask, norm_in, w_proj, w_gate, norm_mid, w_out, form):
    a_side, b_side = lax.map(lambda row_pair: project_row(row_pair[0], row_pair[1], norm_in, w_proj), (z_pair, pair_mask))
    tri_prod = jnp.einsum(form, a_side.astype(jnp.float32), b_side.astype(jnp.float32)).astype(jnp.bfloat16)
    return lax.map(lambda row_pair: output_row(row_pair[0], row_pair[1], norm_in, w_gate, norm_mid, w_out), (z_pair, tri_prod))


def run_crop(z_pair, pair_mask, norm_in, w_proj, w_gate, norm_mid, w_out):
    z_mid = tri_update(z_pair, pair_mask, norm_in[0], w_proj[0], w_gate[0], norm_mid[0], w_out[0], "ikc,jkc->ijc")
    return tri_update(z_mid, pair_mask, norm_in[1], w_proj[1], w_gate[1], norm_mid[1], w_out[1], "kic,kjc->ijc")


def reference(z_one, mask_one, z_two, mask_two, norm_in, w_proj, w_gate, norm_mid, w_out):
    return (run_crop(z_one, mask_one, norm_in, w_proj, w_gate, norm_mid, w_out),
            run_crop(z_two, mask_two, norm_in, w_proj, w_gate, norm_mid, w_out))
```

```python
import functools

import jax
import jax.numpy as jnp
from jax import lax
from jax.experimental import pallas as pl
from jax.experimental.pallas import tpu as pltpu
from jax.sharding import PartitionSpec as P


G = 16
L = 128
F32, BF16 = jnp.float32, jnp.bfloat16
VMEM_BYTES = 63000000


def dot(lhs, rhs):
    return jnp.dot(lhs, rhs, preferred_element_type=F32)


def norm_major(vals, gain, shift):
    scale = 1.0 / vals.shape[0]
    centred = vals - jnp.sum(vals, axis=0, keepdims=True) * scale
    var = jnp.sum(centred * centred, axis=0, keepdims=True) * scale
    return (centred * lax.rsqrt(var + 1e-5) * gain + shift).astype(BF16)


def lanes(tiles):
    return jnp.concatenate([tiles[k] for k in range(tiles.shape[0])], axis=1)


def swap_groups(src, dst, swap):
    width = src.shape[2]
    for g in range(src.shape[1] // G):
        block = src[:, g * G:(g + 1) * G, :].reshape(G * G, width)
        dst[g * G:(g + 1) * G, :, :] = dot(swap, block).astype(BF16).reshape(G, G, width)


def two_stages(first, second):
    n = G // 2

    def both(stage, i):
        for u in range(2):
            stage(2 * i + u)

    def step(i, carry):
        both(second, i)
        both(first, i + 1)
        return carry

    both(first, 0)
    lax.fori_loop(0, n - 1, step, 0)
    both(second, n - 1)


def fetch_rows(z_refs, z_buf, sems):
    step, slots = pl.program_id(0), z_buf.shape[0]
    groups = [ref.at[m * G:(m + 1) * G] for ref in z_refs for m in range(ref.shape[0] // G)]

    def start(k):
        pltpu.make_async_copy(groups[k], z_buf.at[k % slots], sems.at[k % slots]).start()

    @pl.when(step == 0)
    def _():
        start(0)

    for k in range(1, len(groups)):
        @pl.when(step == k - 1)
        def _(k=k):
            start(k)

    slot = lax.rem(step, slots)
    pltpu.make_async_copy(groups[0], z_buf.at[slot], sems.at[slot]).wait()
    return slot


def project_kernel(n, unread, *refs):
    z_refs, refs = refs[:n], refs[n:]
    mask, gain, shift, w_t, swap = refs[:5]
    refs = refs[5 + unread:]
    a_out, x_out, b_out, z_buf, a_scr, b_scr, sems = refs
    slot = fetch_rows(z_refs, z_buf, sems)
    cols, chan = z_buf.shape[2:]

    def normed(r):
        for k in range(cols // L):
            z_t = z_buf[slot, r, k * L:(k + 1) * L, :].astype(F32).T
            x_out[r, k] = norm_major(z_t, gain[...], shift[...])

    def gated(r):
        x = lanes(x_out[r])
        keep = mask[pl.ds(r, 1), :]
        for side, scr in ((0, a_scr), (1, b_scr)):
            w0 = side * 2 * chan
            val = dot(w_t[w0:w0 + chan, :], x)
            gate = dot(w_t[w0 + chan:w0 + 2 * chan, :], x)
            scr[r] = (val * keep * (jnp.tanh(gate) + 1.0)).astype(BF16)

    two_stages(normed, gated)
    swap_groups(a_scr, a_out, swap[...])
    swap_groups(b_scr, b_out, swap[...])


def project(z_list, mask, start, total, prev, gain, shift, w_t, swap, after=()):
    n_refs, n = len(z_list), sum(arr.shape[0] for arr in z_list) // G
    _, cols, chan = z_list[0].shape
    any_spec = pl.BlockSpec(memory_space=pl.ANY)
    whole = lambda arr: pl.BlockSpec(arr.shape, lambda g: (0,) * arr.ndim)
    aliased = 0 if prev is None else 2
    return pl.pallas_call(
        functools.partial(project_kernel, n_refs, aliased + len(after)),
        grid=(n,),
        in_specs=[any_spec] * n_refs + [pl.BlockSpec((G, cols), lambda g: (g, 0)), whole(gain), whole(shift), whole(w_t), whole(swap)]
        + [any_spec] * (aliased + len(after)),
        out_specs=[pl.BlockSpec((chan, G, cols), lambda g: (0, start + g, 0)),
                   pl.BlockSpec((G, cols // L, chan, L), lambda g: (start + g, 0, 0, 0)),
                   pl.BlockSpec((chan, G, cols), lambda g: (0, g, 0))],
        out_shape=[jax.ShapeDtypeStruct((chan, total, cols), BF16),
                   jax.ShapeDtypeStruct((total, cols // L, chan, L), BF16),
                   jax.ShapeDtypeStruct((chan, n * G, cols), BF16)],
        scratch_shapes=[pltpu.VMEM((2, G, cols, chan), BF16), pltpu.VMEM((G, chan, cols), BF16),
                        pltpu.VMEM((G, chan, cols), BF16), pltpu.SemaphoreType.DMA((2,))],
        input_output_aliases={} if prev is None else {n_refs + 5: 0, n_refs + 6: 1},
        compiler_params=pltpu.CompilerParams(vmem_limit_bytes=VMEM_BYTES, dimension_semantics=("arbitrary",)),
        cost_estimate=pl.CostEstimate(flops=n * 6 * 10**9, bytes_accessed=n * 8 * 2**20, transcendentals=0),
        name="project_rows",
    )(*z_list, mask, gain, shift, w_t, swap, *(prev or ()), *after)


def outgoing_kernel(sizes, where, *refs):
    n = len(sizes)
    a_ref, own, other, swap = refs[0], refs[1:1 + n], refs[1 + n:1 + 2 * n], refs[1 + 2 * n]
    t_out, t_scr, b_scr = refs[2 + 2 * n:]
    width = t_scr.shape[2]

    def channel(c, carry):
        for side, parts in ((0, own), (1, other)):
            m = 0
            for size, part in zip(sizes, parts):
                for g in range(size):
                    b_scr[where[side, m]] = part[c, g * G:(g + 1) * G, :]
                    m += 1
        b_mat = b_scr[...].reshape(-1, b_scr.shape[2])
        t_scr[c] = lax.dot_general(a_ref[c], b_mat, (((1,), (1,)), ((), ())), preferred_element_type=F32).astype(BF16)
        return carry

    lax.fori_loop(0, G, channel, 0, unroll=2)

    def group(i, carry):
        rows = pl.ds(pl.multiple_of(i * G, G), G)
        block = t_scr[:, rows, :].reshape(G * G, width)
        res = dot(swap[...], block).astype(BF16).reshape(G, G, width)
        for k in range(width // L):
            t_out[0, rows, k] = res[:, :, k * L:(k + 1) * L]
        return carry

    lax.fori_loop(0, t_scr.shape[1] // G, group, 0)


def outgoing(where, a, own, other, swap):
    chan, rows, cols = a.shape
    sizes = tuple(b.shape[1] // G for b in own)
    width = 2 * rows
    spec = lambda n_rows: pl.BlockSpec((G, n_rows, cols), lambda g, w: (g, 0, 0))
    return pl.pallas_call(
        functools.partial(outgoing_kernel, sizes),
        grid_spec=pltpu.PrefetchScalarGridSpec(
            num_scalar_prefetch=1, grid=(chan // G,),
            in_specs=[spec(rows)] + [spec(b.shape[1]) for b in own] + [spec(b.shape[1]) for b in other]
            + [pl.BlockSpec(swap.shape, lambda g, w: (0, 0))],
            out_specs=pl.BlockSpec((1, rows, width // L, G, L), lambda g, w: (g, 0, 0, 0, 0)),
            scratch_shapes=[pltpu.VMEM((G, rows, width), BF16), pltpu.VMEM((width // G, G, cols), BF16)]),
        out_shape=jax.ShapeDtypeStruct((chan // G, rows, width // L, G, L), BF16),
        compiler_params=pltpu.CompilerParams(vmem_limit_bytes=VMEM_BYTES, dimension_semantics=("arbitrary",)),
        cost_estimate=pl.CostEstimate(flops=40 * 10**9, bytes_accessed=128 * 2**20, transcendentals=0),
        name="outgoing_product",
    )(where, a, *own, *other, swap)


def finish_row(z_t, t_row, x, norm, w_out_t, w_gate_t, put):
    n_tiles = x.shape[1] // L
    y = jnp.concatenate([norm_major(t_row(k), norm[0], norm[1]) for k in range(n_tiles)], axis=1)
    update = dot(w_out_t, y)
    gate = jnp.tanh(dot(w_gate_t, x)) + 1.0
    for k in range(n_tiles):
        ks = slice(k * L, (k + 1) * L)
        put(k, (z_t(k) + gate[:, ks] * update[:, ks]).astype(BF16))


def middle_kernel(n, aliased, keep_mid, tile, *refs):
    z_refs, refs = refs[:n], refs[n:]
    t_ref, x_ref, mask, norms, w_out_t, w_gate_t, w_t, swap = refs[:8]
    refs = refs[8 + aliased:]
    a_out, b_out, done = refs[:3]
    mid_out = refs[3] if keep_mid else None
    done[...] = jnp.zeros_like(done)
    z_buf, x_scr, a_scr, b_scr, keep_scr, sems = refs[3 + keep_mid:]
    slot = fetch_rows(z_refs, z_buf, sems)
    chan = z_buf.shape[3]
    tile_cols = pl.ds(pl.multiple_of(tile[0] * L, L), L)
    keep_scr[...] = mask[:, tile_cols]

    def updated(r):
        def put(k, z_mid):
            if keep_mid:
                mid_out[r, k] = z_mid
            x_scr[r, k] = norm_major(z_mid.astype(F32), norms[2], norms[3])

        finish_row(lambda k: z_buf[slot, r, k * L:(k + 1) * L, :].astype(F32).T, lambda k: t_ref[:, r, k].reshape(chan, L).astype(F32), lanes(x_ref[r]),
                   (norms[0], norms[1]), w_out_t[...], w_gate_t[...], put)

    def gated(r):
        x_mid, x_tile = lanes(x_scr[r]), x_scr[r, tile[0]]
        b_val, b_gate = dot(w_t[2 * chan:3 * chan, :], x_mid), dot(w_t[3 * chan:, :], x_mid)
        b_scr[r] = (b_val * mask[pl.ds(r, 1), :] * (jnp.tanh(b_gate) + 1.0)).astype(BF16)
        a_val, a_gate = dot(w_t[:chan, :], x_tile), dot(w_t[chan:2 * chan, :], x_tile)
        a_scr[r] = (a_val * keep_scr[pl.ds(r, 1), :] * (jnp.tanh(a_gate) + 1.0)).astype(BF16)

    two_stages(updated, gated)
    swap_groups(a_scr, a_out, swap[...])
    swap_groups(b_scr, b_out, swap[...])


def middle(tile, z_list, t, x, mask, start, prev, norms, w_out_t, w_gate_t, w_t, swap, keep_mid):
    n_refs, n = len(z_list), sum(arr.shape[0] for arr in z_list) // G
    _, cols, chan = z_list[0].shape
    total = t.shape[1]
    any_spec = pl.BlockSpec(memory_space=pl.ANY)
    whole = lambda arr: pl.BlockSpec(arr.shape, lambda g, s: (0,) * arr.ndim)
    rows_spec = pl.BlockSpec((G, cols // L, chan, L), lambda g, s: (start + g, 0, 0, 0))
    t_spec = pl.BlockSpec((chan // G, G, cols // L, G, L), lambda g, s: (0, start + g, 0, 0, 0))
    aliased = 0 if prev is None else 2
    out_specs = [pl.BlockSpec((chan, G, L), lambda g, s: (0, start + g, 0)),
                 pl.BlockSpec((chan, G, cols), lambda g, s: (0, start + g, 0)), pl.BlockSpec((8, L), lambda g, s: (0, 0))]
    out_shape = [jax.ShapeDtypeStruct((chan, total, L), BF16), jax.ShapeDtypeStruct((chan, total, cols), BF16),
                 jax.ShapeDtypeStruct((8, L), F32)]
    if keep_mid:
        out_specs.append(pl.BlockSpec((G, cols // L, chan, L), lambda g, s: (g, 0, 0, 0)))
        out_shape.append(jax.ShapeDtypeStruct((n * G, cols // L, chan, L), BF16))

    def kernel(tile_ref, *refs):
        middle_kernel(n_refs, aliased, keep_mid, tile_ref, *refs)

    return pl.pallas_call(
        kernel,
        grid_spec=pltpu.PrefetchScalarGridSpec(
            num_scalar_prefetch=1, grid=(n,),
            in_specs=[any_spec] * n_refs + [t_spec, rows_spec, pl.BlockSpec((G, cols), lambda g, s: (g, 0)), whole(norms),
                                       whole(w_out_t), whole(w_gate_t), whole(w_t), whole(swap)] + [any_spec] * aliased,
            out_specs=out_specs,
            scratch_shapes=[pltpu.VMEM((2, G, cols, chan), BF16), pltpu.VMEM((G, cols // L, chan, L), BF16), pltpu.VMEM((G, chan, L), BF16),
                            pltpu.VMEM((G, chan, cols), BF16), pltpu.VMEM((G, L), F32), pltpu.SemaphoreType.DMA((2,))]),
        out_shape=out_shape,
        input_output_aliases={} if prev is None else {n_refs + 9: 0, n_refs + 10: 1},
        compiler_params=pltpu.CompilerParams(vmem_limit_bytes=VMEM_BYTES, dimension_semantics=("arbitrary",)),
        cost_estimate=pl.CostEstimate(flops=n * 7 * 10**9, bytes_accessed=n * 10 * 2**20, transcendentals=0),
        name="middle_rows",
    )(tile, *z_list, t, x, mask, norms, w_out_t, w_gate_t, w_t, swap, *(prev or ()))


def incoming_kernel(own_rows, place, a_ref, b_ref, own_out, other_out, scr):
    def channel(c, carry):
        scr[...] = lax.dot_general(a_ref[c], b_ref[c], (((0,), (0,)), ((), ())), preferred_element_type=F32)
        own_out[c] = scr[pl.ds(pl.multiple_of(place[0] * own_rows, own_rows), own_rows), :]
        other_out[c] = scr[pl.ds(pl.multiple_of(place[1] * own_rows, own_rows), own_rows), :]
        return carry

    lax.fori_loop(0, G, channel, 0, unroll=2)


def incoming(place, a, b, own_rows):
    chan, rows, cols = b.shape
    out = jax.ShapeDtypeStruct((chan, own_rows, cols), F32)
    out_spec = pl.BlockSpec((G, own_rows, cols), lambda g, s: (g, 0, 0))
    return pl.pallas_call(
        functools.partial(incoming_kernel, own_rows),
        grid_spec=pltpu.PrefetchScalarGridSpec(
            num_scalar_prefetch=1, grid=(chan // G,),
            in_specs=[pl.BlockSpec((G, rows, L), lambda g, s: (g, 0, 0)), pl.BlockSpec((G, rows, cols), lambda g, s: (g, 0, 0))],
            out_specs=[out_spec, out_spec],
            scratch_shapes=[pltpu.VMEM((L, cols), F32)]),
        out_shape=[out, out],
        compiler_params=pltpu.CompilerParams(vmem_limit_bytes=VMEM_BYTES, dimension_semantics=("arbitrary",)),
        cost_estimate=pl.CostEstimate(flops=20 * 10**9, bytes_accessed=60 * 2**20, transcendentals=0),
        name="incoming_product",
    )(place, a, b)


def last_kernel(own, other, mid, norms, w_out_t, w_gate_t, swap, z_out, t_scr, x_scr):
    chan, rows, cols = own.shape
    for g in range(chan // G):
        cs = slice(g * G, (g + 1) * G)
        block = (own[cs] + other[cs]).astype(BF16).reshape(G * rows, cols)
        res = dot(swap[...], block).astype(BF16).reshape(G, G, cols)
        for k in range(cols // L):
            t_scr[:, k, cs, :] = res[:, :, k * L:(k + 1) * L]

    def row(r, carry):
        for k in range(cols // L):
            x_scr[k] = norm_major(mid[r, k].astype(F32), norms[2], norms[3])

        def put(k, z_new):
            z_out[r, k * L:(k + 1) * L, :] = z_new.astype(F32).T.astype(BF16)

        finish_row(lambda k: mid[r, k].astype(F32), lambda k: t_scr[r, k].astype(F32), lanes(x_scr[...]),
                   (norms[0], norms[1]), w_out_t[...], w_gate_t[...], put)
        return carry

    lax.fori_loop(0, G, row, 0, unroll=2)


def last(own, other, mid, norms, w_out_t, w_gate_t, swap):
    chan, rows, cols = own.shape
    whole = lambda arr: pl.BlockSpec(arr.shape, lambda g: (0,) * arr.ndim)
    part = pl.BlockSpec((chan, G, cols), lambda g: (0, g, 0))
    return pl.pallas_call(
        last_kernel,
        grid=(rows // G,),
        in_specs=[part, part, pl.BlockSpec((G, cols // L, chan, L), lambda g: (g, 0, 0, 0)), whole(norms), whole(w_out_t), whole(w_gate_t),
                  whole(swap)],
        out_specs=pl.BlockSpec((G, cols, chan), lambda g: (g, 0, 0)),
        out_shape=jax.ShapeDtypeStruct((rows, cols, chan), BF16),
        scratch_shapes=[pltpu.VMEM((G, cols // L, chan, L), BF16), pltpu.VMEM((cols // L, chan, L), BF16)],
        compiler_params=pltpu.CompilerParams(vmem_limit_bytes=VMEM_BYTES, dimension_semantics=("arbitrary",)),
        cost_estimate=pl.CostEstimate(flops=20 * 10**9, bytes_accessed=32 * 2**20, transcendentals=0),
        name="last_rows",
    )(own, other, mid, norms, w_out_t, w_gate_t, swap)


def ring_perms(size):
    step = lambda d: [(i, (i + d) % size) for i in range(size)]
    return step(2), step(-2), [(i, i ^ 1) for i in range(size)]


def hop(arr, perm):
    return lax.ppermute(arr, "dap", perm)


def gather_steps(rows, size):
    right, left, _ = ring_perms(size)
    last_hop = size // 4
    from_left = from_right = rows
    steps = [[(0, 0, rows)]]
    for s in range(1, last_hop):
        from_left, from_right = hop(from_left, right), hop(from_right, left)
        steps.append([(s, 0, from_left), (-s, 0, from_right)])
    half = rows.shape[0] // 2
    steps.append([(last_hop, 0, hop(from_left[:half], right)),
                  (last_hop, half // G, hop(from_right[half:], left))])
    return steps


def solution(mesh):
    size = mesh.shape["dap"]
    chips = size // 2
    row_spec = P(("data", "dap"), None, None)
    mask_spec = P(("data", "dap"), None)

    def per_device(z_one, mask_one, z_two, mask_two, norm_in, w_proj, w_gate, norm_mid, w_out):
        me = lax.axis_index("dap")
        chip, core = me // 2, me % 2
        own_rows, _, chan = z_one.shape
        n_piece = own_rows // G
        swap_row = lax.broadcasted_iota(jnp.int32, (G * G, G * G), 0)
        swap_col = lax.broadcasted_iota(jnp.int32, (G * G, G * G), 1)
        swap = ((swap_row // G == swap_col % G) & (swap_row % G == swap_col // G)).astype(BF16)
        spread = lambda vec: jnp.broadcast_to(vec.astype(F32)[..., None], vec.shape + (L,))
        gains_in, gains_mid = spread(norm_in), spread(norm_mid)
        gate_half = jnp.tile(jnp.repeat(jnp.array([1.0, 0.5], BF16), chan), 2)
        w_proj_t = jnp.swapaxes(w_proj * gate_half, 1, 2)
        w_gate_t = jnp.swapaxes(w_gate * jnp.array(0.5, BF16), 1, 2)
        w_out_t = jnp.swapaxes(w_out * jnp.array(0.5, BF16), 1, 2)
        tile = (chip * 2 * own_rows // L).reshape(1).astype(jnp.int32)
        in_tile = chip * 2 % (L // own_rows)
        place = jnp.stack([in_tile + core, in_tile + 1 - core]).astype(jnp.int32)
        _, _, partner = ring_perms(size)

        half_masks = jnp.stack([mask_one, mask_two]).astype(BF16) * 0.5
        mask_from = {d: hop(half_masks, [(i, (i + 2 * d) % size) for i in range(size)]) for d in range(1, chips)}
        mask_from[0] = half_masks

        z_steps = [gather_steps(z_one, size)]
        behind = [arr for _, _, arr in z_steps[0][chips // 2 - 1]]
        z_steps.append(gather_steps(lax.optimization_barrier((z_two, *behind))[0], size))

        places = []
        for side in (core, 1 - core):
            places.append(jnp.stack([((chip - dist) % chips * 2 + side) * n_piece + m for step in z_steps[0]
                                     for dist, first, arr in step for m in range(first, first + arr.shape[0] // G)]))
        where = jnp.stack(places).astype(jnp.int32)

        norms_mid = jnp.stack([gains_mid[0, 0], gains_mid[0, 1], gains_in[1, 0], gains_in[1, 1]])
        norms_last = jnp.stack([gains_mid[1, 0], gains_mid[1, 1], gains_in[1, 0], gains_in[1, 1]])
        step_rows = [sum(arr.shape[0] for _, _, arr in step) for step in z_steps[0]]
        starts = [sum(step_rows[:s]) // G for s in range(len(step_rows))]
        total = sum(step_rows)

        def first_half(crop, masks, after):
            prev, own_b, other_b = None, [], []
            for s, step in enumerate(z_steps[crop]):
                a, x, b = project([arr for _, _, arr in step], masks[s], starts[s], total, prev,
                                  gains_in[0, 0], gains_in[0, 1], w_proj_t[0], swap, after[s])
                prev = (a, x)
                own_b.append(b)
                other_b.append(hop(b, partner))
            return a, x, own_b, other_b

        def second_half(crop, masks, a, x, own_b, other_b):
            t = outgoing(where, a, own_b, other_b, swap)
            prev, mid, done = None, None, []
            for s, step in enumerate(z_steps[crop]):
                res = middle(tile, [arr for _, _, arr in step], t, x, masks[s], starts[s], prev, norms_mid,
                             w_out_t[0], w_gate_t[0], w_proj_t[1], swap, s == 0)
                prev = tuple(res[:2])
                mid = res[3] if s == 0 else mid
                done.append(res[2])
            own_t, other_t = incoming(place, prev[0], prev[1], own_rows)
            got_t = hop(other_t, partner)
            return t, done, own_t, last(own_t, got_t, mid, norms_last, w_out_t[1], w_gate_t[1], swap)

        masks = [[jnp.concatenate([mask_from[dist % chips][crop, first * G:first * G + arr.shape[0]] for dist, first, arr in step]).astype(F32)
                  for step in z_steps[0]] for crop in range(2)]
        n_steps = len(starts)
        t, done, own_t, out_one = second_half(0, masks[0], *first_half(0, masks[0], [()] * n_steps))
        behind = [t] + done[1::2][:n_steps - 3] + [own_t, out_one]
        out_two = second_half(1, masks[1], *first_half(1, masks[1], [(arr,) for arr in behind]))[3]
        return out_one, out_two

    return jax.shard_map(per_device, mesh=mesh,
                         in_specs=(row_spec, mask_spec, row_spec, mask_spec, P(), P(), P(), P(), P()),
                         out_specs=(row_spec, row_spec), check_vma=False)
```
